32 devices in a mesh: clip: 4 (over x, core), tx: 4 (over z), ty: 2 (over y).
Axes of the slice: x: 2, y: 2, z: 4, core: 2. Of those that a mesh axis runs over, the one named last changes fastest.
Arguments:
- query_states: bfloat16 [32, 128, 1152], P(('clip', 'tx', 'ty')), parts along dimension 0, may hold values from -64 to 64
- key_states: bfloat16 [32, 128, 1152], P(('clip', 'tx', 'ty')), parts along dimension 0, may hold values from -24 to 24
- value_states: bfloat16 [32, 128, 1152], P(('clip', 'tx', 'ty')), parts along dimension 0, may hold values from -6 to 6
- grad_output: bfloat16 [32, 128, 1152], P(('clip', 'tx', 'ty')), parts along dimension 0, may hold values from -6 to 6
- branch_gate: float32 [4608], P('clip'), parts along dimension 0, may hold values from 0.1 to 1.9
- out_weight: bfloat16 [1152, 1152], P('tx'), may hold values from -0.1875 to 0.1875
Outputs:
- query_grad: bfloat16 [32, 128, 1152], P(('clip', 'tx', 'ty')), parts along dimension 0
- key_grad: bfloat16 [32, 128, 1152], P(('clip', 'tx', 'ty')), parts along dimension 0
- value_grad: bfloat16 [32, 128, 1152], P(('clip', 'tx', 'ty')), parts along dimension 0
- gate_grad: float32 [4608], P('clip'), parts along dimension 0
The draws below stay inside these ranges and needn't reach their ends.
There are 4 independent parts, one for each index of `clip`. The reference program is written for one: setup_inputs(seed, part) draws one part's arguments, and reference() takes and returns one part's arrays. A program takes and returns all parts, laid end to end along the dimension named above; an argument that names none is the same for every part. Nothing has to cross between parts.
All inputs are finite; a program needn't handle non-finite values.
Results may differ from the reference program's by a relative error of at most 0.025.
Values may be sent and summed in bfloat16 or wider, within the bound.
A program may use at most 64 MiB of HBM per device.

```python
import jax
import jax.numpy as jnp
from jax import lax

HEADS = 16
HEAD_DIM = 72
D = 1152
POS = 128
FRAMES = 8


def paired_draw(key):
    base = jax.random.fold_in(key, 4242)
    key_q, key_k = jax.random.split(base, 2)
    shape = (FRAMES, POS, D)
    queries = jnp.clip(jax.random.normal(key_q, shape, jnp.float32), -6.0, 6.0)
    keys_out = jnp.clip(jax.random.normal(key_k, shape, jnp.float32), -6.0, 6.0)
    return (queries, keys_out)


def draw_query_states(key, part):
    return paired_draw(key)[0].astype(jnp.bfloat16)


def draw_key_states(key, part):
    return paired_draw(key)[1].astype(jnp.bfloat16)


def steps_of(rng, dims, pieces, least, largest):
    gain = 1.0
    for axis_at, parts in pieces:
        steps = jax.random.uniform(jax.random.fold_in(jax.random.fold_in(rng, 6), axis_at), (parts,), jnp.float32, least / len(pieces), largest / len(pieces))
        gain = gain * jnp.repeat(jnp.exp(steps), dims[axis_at] // parts).reshape((-1,) + (1,) * (len(dims) - 1 - axis_at))
    return gain


def gaussian(stream_key, shape, deviation, reach, cuts=(), dtype=jnp.bfloat16):
    entries = jax.random.normal(stream_key, shape, jnp.float32) * deviation
    if len(cuts) > 0:
        entries = steps_of(stream_key, shape, cuts, -0.22, 0.18) * entries
    return jnp.clip(entries, min=-reach, max=reach).astype(dtype)


def setup_inputs(seed: int = 0, part: int = 0) -> dict:
    keys = jax.random.split(jax.random.key(seed), 7)
    own_keys = jax.random.split(jax.random.fold_in(keys[6], part), 7)
    return {
        "query_states": draw_query_states(jax.random.fold_in(jax.random.fold_in(keys[6], part), 71), part),
        "key_states": draw_key_states(jax.random.fold_in(jax.random.fold_in(keys[6], part), 71), part),
        "value_states": gaussian(own_keys[2], (FRAMES, POS, D), 1.0, 6.0, ((0, 8),)),
        "grad_output": gaussian(own_keys[3], (FRAMES, POS, D), 1.0, 6.0, ((0, 8),)),
        "branch_gate": jnp.clip(1.0 + 0.18 * jax.random.normal(own_keys[4], (D,), jnp.float32), 0.1, 1.9),
        "out_weight": gaussian(keys[5], (D, D), D ** -0.5, 0.1875, ((0, 4),)),
    }


def one_position(operands):
    queries, keys_in, values_in, grads_in = operands
    shape4 = (FRAMES, HEADS, HEAD_DIM)
    q_f = queries.reshape(shape4).astype(jnp.float32)
    k_f = keys_in.reshape(shape4).astype(jnp.float32)
    v_f = values_in.reshape(shape4).astype(jnp.float32)
    g_f = grads_in.reshape(shape4).astype(jnp.float32)
    factor = HEAD_DIM ** -0.5
    scores = jnp.einsum('fhd,ghd->hfg', q_f, k_f) * factor
    peak = jnp.max(scores, axis=-1, keepdims=True)
    expon = jnp.exp(scores - peak)
    probs = expon / jnp.sum(expon, axis=-1, keepdims=True)
    probs_b = probs.astype(jnp.bfloat16).astype(jnp.float32)
    attn_out = jnp.einsum('hfg,ghd->fhd', probs_b, v_f).astype(jnp.bfloat16)
    value_grad = jnp.einsum('hfg,fhd->ghd', probs_b, g_f).astype(jnp.bfloat16)
    dprobs = jnp.einsum('fhd,ghd->hfg', g_f, v_f)
    delta = jnp.sum(g_f * attn_out.astype(jnp.float32), axis=-1)
    delta = jnp.transpose(delta, (1, 0))[:, :, None]
    dscores = (probs * (dprobs - delta) * factor).astype(jnp.bfloat16).astype(jnp.float32)
    query_grad = jnp.einsum('hfg,ghd->fhd', dscores, k_f).astype(jnp.bfloat16)
    key_grad = jnp.einsum('hfg,fhd->ghd', dscores, q_f).astype(jnp.bfloat16)
    flat = (FRAMES, D)
    return (query_grad.reshape(flat), key_grad.reshape(flat), value_grad.reshape(flat), attn_out.reshape(flat))


def reference(query_states, key_states, value_states, grad_output, branch_gate, out_weight):
    gated = (grad_output.astype(jnp.float32) * branch_gate).astype(jnp.bfloat16)
    d_attn = jnp.dot(gated.reshape(FRAMES * POS, D), out_weight.T, preferred_element_type=jnp.float32)
    d_attn = d_attn.astype(jnp.bfloat16).reshape(FRAMES, POS, D)
    operands = tuple(jnp.transpose(arr, (1, 0, 2)) for arr in (query_states, key_states, value_states, d_attn))
    results = lax.map(one_position, operands)
    query_grad, key_grad, value_grad, attn_out = tuple(jnp.transpose(arr, (1, 0, 2)) for arr in results)
    branch_out = jnp.dot(attn_out.reshape(FRAMES * POS, D), out_weight, preferred_element_type=jnp.float32)
    gate_grad = jnp.sum(grad_output.reshape(FRAMES * POS, D).astype(jnp.float32) * branch_out, axis=0)
    return query_grad, key_grad, value_grad, gate_grad
```

```python
import functools

import jax
import jax.numpy as jnp
from jax import lax
from jax.experimental import pallas as pl
from jax.experimental.pallas import tpu as pltpu
from jax.sharding import PartitionSpec as P

HEAD_DIM = 72


def shortened(x):

    def short(part):
        return part.astype(jnp.bfloat16) if part.dtype == jnp.float32 else part

    return jax.tree.map(short, x)


def attend_block(queries, keys_in, values_in, grads_in):
    frames, block_pos, block_width = queries.shape
    heads_here = block_width // HEAD_DIM
    shape4 = (frames, block_pos, heads_here, HEAD_DIM)
    q_four = queries.reshape(shape4)
    k_four = keys_in.reshape(shape4)
    v_four = values_in.reshape(shape4)
    g_four = grads_in.reshape(shape4)
    factor = HEAD_DIM ** (-0.5)
    scores = (
        jnp.einsum("fphd,gphd->phfg", q_four, k_four, preferred_element_type=jnp.float32) * factor
    )
    peak = jnp.max(scores, axis=-1, keepdims=True)
    expon = jnp.exp(scores - peak)
    probs = expon / jnp.sum(expon, axis=-1, keepdims=True)
    probs_b = probs.astype(jnp.bfloat16)
    attn_out = jnp.einsum(
        "phfg,gphd->fphd", probs_b, v_four, preferred_element_type=jnp.float32
    ).astype(jnp.bfloat16)
    value_grad = jnp.einsum(
        "phfg,fphd->gphd", probs_b, g_four, preferred_element_type=jnp.float32
    ).astype(jnp.bfloat16)
    dprobs = jnp.einsum("fphd,gphd->phfg", g_four, v_four, preferred_element_type=jnp.float32)
    delta = jnp.sum(g_four.astype(jnp.float32) * attn_out.astype(jnp.float32), axis=-1)
    delta = jnp.transpose(delta, (1, 2, 0))[..., None]
    dscores = (probs * (dprobs - delta) * factor).astype(jnp.bfloat16)
    query_grad = jnp.einsum(
        "phfg,gphd->fphd", dscores, k_four, preferred_element_type=jnp.float32
    ).astype(jnp.bfloat16)
    key_grad = jnp.einsum(
        "phfg,fphd->gphd", dscores, q_four, preferred_element_type=jnp.float32
    ).astype(jnp.bfloat16)
    flat = (frames, block_pos, block_width)
    return (
        query_grad.reshape(flat),
        key_grad.reshape(flat),
        value_grad.reshape(flat),
        attn_out.reshape(flat),
    )


def split_for_direct(array, across_x, across_y):
    positions, width = array.shape
    pieces = array.reshape(across_y, positions // across_y, across_x, width // across_x)
    pieces = jnp.transpose(pieces, (2, 0, 1, 3))
    return pieces.reshape(1, across_x * across_y, positions // across_y, width // across_x)


def join_from_direct(array, across_x, across_y):
    block_pos, block_width = (array.shape[2], array.shape[3])
    pieces = array.reshape(across_x, across_y, block_pos, block_width)
    pieces = jnp.transpose(pieces, (1, 2, 0, 3))
    return pieces.reshape(1, across_y * block_pos, across_x * block_width)


def per_device_plain(query_states, key_states, value_states, grad_output, branch_gate, out_weight):
    across_x = lax.axis_size("tx")
    across_y = lax.axis_size("ty")
    devices_here = across_x * across_y
    positions = grad_output.shape[1]
    width = grad_output.shape[2]
    block_pos = positions // across_y
    block_width = width // across_x
    grad_rows = grad_output[0]
    gated = (grad_rows.astype(jnp.float32) * branch_gate).astype(jnp.bfloat16)
    d_attn = lax.dot_general(
        gated,
        lax.all_gather(out_weight, "tx", axis=0, tiled=True),
        (((1,), (1,)), ((), ())),
        preferred_element_type=jnp.float32,
    )
    d_attn = d_attn.astype(jnp.bfloat16)
    sources = (query_states[0], key_states[0], value_states[0], d_attn)
    prepared = tuple((split_for_direct(arr, across_x, across_y) for arr in sources))
    moved = jax.tree.map(
        lambda part, own: part.astype(own.dtype),
        lax.all_to_all(shortened(prepared), ("tx", "ty"), split_axis=1, concat_axis=0, tiled=True),
        prepared,
    )
    moved = tuple((arr.reshape(devices_here, block_pos, block_width) for arr in moved))
    results = attend_block(moved[0], moved[1], moved[2], moved[3])
    outgoing = tuple((arr.reshape(devices_here, 1, block_pos, block_width) for arr in results))
    returned = jax.tree.map(
        lambda part, own: part.astype(own.dtype),
        lax.all_to_all(shortened(outgoing), ("tx", "ty"), split_axis=0, concat_axis=1, tiled=True),
        outgoing,
    )
    returned = tuple((join_from_direct(arr, across_x, across_y) for arr in returned))
    query_grad, key_grad, value_grad, attn_frame = returned
    attn_rows = attn_frame[0]
    branch_out = jnp.dot(
        attn_rows,
        lax.all_gather(out_weight, "tx", axis=0, tiled=True),
        preferred_element_type=jnp.float32,
    )
    local_terms = jnp.sum(grad_rows.astype(jnp.float32) * branch_out, axis=0)
    gate_grad = lax.psum(local_terms, ("tx", "ty"))
    return (query_grad, key_grad, value_grad, gate_grad)


LANES = 128
MESH = pl.DeviceIdType.MESH
NT = (((1,), (1,)), ((), ()))
TN = (((0,), (0,)), ((), ()))


def dot(a, b, dims=(((1,), (0,)), ((), ()))):
    return lax.dot_general(a, b, dims, preferred_element_type=jnp.float32)


def pack(rows, across_x, block_width, group):
    full = block_width // LANES
    rest = block_width % LANES
    groups = LANES // rest
    block_pos = group * groups
    blocks = []
    for t in range(across_x):
        base = t * block_width
        tiles = [rows[:, base + j * LANES : base + (j + 1) * LANES] for j in range(full)]
        narrow = rows[:, base + full * LANES : base + block_width]
        for u in range(rows.shape[0] // block_pos):
            start = u * block_pos
            parts = [tile[start : start + block_pos] for tile in tiles]
            parts.append(
                jnp.concatenate(
                    [narrow[start + g * group : start + (g + 1) * group] for g in range(groups)], axis=1
                )
            )
            blocks.append((t, u, parts))
    return blocks


def fused_kernel(
    across_x, across_y, block_width, group,
    q_ref, k_ref, v_ref, g_ref, gate_ref, w_ref,
    dq_ref, dk_ref, dv_ref, gg_ref,
    send_pack, recv_pack, recv_g, out_pack, ret_pack, w_aug, gate_own, gate_all,
    fs, fr, gs, gr, rs, rr, ps, pr,
):
    n = across_x * across_y
    mx, my = lax.axis_index("tx"), lax.axis_index("ty")
    me = mx * across_y + my
    full = block_width // LANES
    rest = block_width % LANES
    groups = LANES // rest
    block_pos = group * groups
    tiles = full + 1
    rows = n * group
    heads = block_width // HEAD_DIM
    factor = HEAD_DIM ** (-0.5)

    def ident(d):
        return {"tx": d // across_y, "ty": d % across_y}

    def other(o):
        return lax.rem(me + o, n)

    barrier = pltpu.get_barrier_semaphore()
    for o in range(1, n):
        pl.semaphore_signal(barrier, inc=1, device_id=ident(other(o)), device_id_type=MESH)
    pl.semaphore_wait(barrier, n - 1)

    def remote(src, dst, ss, sr, d):
        return pltpu.make_async_remote_copy(
            src_ref=src, dst_ref=dst, send_sem=ss, recv_sem=sr, device_id=ident(d), device_id_type=MESH
        )

    started = []
    for o in range(1, n):
        d = other(o)
        copy = remote(g_ref.at[d % across_y], recv_g.at[me], gs.at[d], gr.at[me], d)
        copy.start()
        started.append(copy)
    for a, ref in enumerate((q_ref, k_ref, v_ref)):
        for t, u, parts in pack(ref[...], across_x, block_width, group):
            d = t * across_y + u
            for j, part in enumerate(parts):
                send_pack[a, d, j * block_pos : j * block_pos + part.shape[0], :] = part
        for o in range(1, n):
            d = other(o)
            copy = remote(send_pack.at[a, d], recv_pack.at[a, me], fs.at[a, d], fr.at[a, me], d)
            copy.start()
            started.append(copy)
        recv_pack[a, me] = send_pack[a, me]
    recv_g[me] = g_ref[my]
    w_aug[: full * LANES, :] = w_ref[: full * LANES, :]
    for g in range(groups):
        w_aug[full * LANES + g * rest : full * LANES + (g + 1) * rest, :] = w_ref[full * LANES :, :]
    for a in range(3):
        out_pack[a, :, full * block_pos :, :] = jnp.zeros((n, group, LANES), jnp.bfloat16)
    gate_own[...] = jnp.zeros_like(gate_own)

    for o in range(1, n):
        s = other(o)
        remote(recv_g.at[s], recv_g.at[s], gs.at[s], gr.at[s], s).wait_recv()
        for a in range(3):
            remote(recv_pack.at[a, s], recv_pack.at[a, s], fs.at[a, s], fr.at[a, s], s).wait_recv()

    lane = lax.broadcasted_iota(jnp.int32, (1, tiles * LANES), 1)
    row_pos = lax.broadcasted_iota(jnp.int32, (rows, rows), 0) % group
    col_pos = lax.broadcasted_iota(jnp.int32, (rows, rows), 1) % group
    same = row_pos == col_pos

    def one_group(g, carry):
        start = pl.multiple_of(g * group, group)
        tail = lane - full * LANES
        channel = jnp.where(
            tail < 0, lane, jnp.where(tail // rest == g, full * LANES + tail % rest, block_width)
        )
        head_of = channel // HEAD_DIM

        def load(a):
            parts = []
            for j in range(full):
                at = pl.multiple_of(j * block_pos + start, group)
                parts.append(recv_pack[a, :, pl.ds(at, group), :].reshape(rows, LANES))
            parts.append(recv_pack[a, :, full * block_pos :, :].reshape(rows, LANES))
            return parts

        qt, kt, vt = load(0), load(1), load(2)
        grads = recv_g[:, pl.ds(start, group), :].reshape(rows, recv_g.shape[2]).astype(jnp.float32)
        gated = (grads * gate_ref[...]).astype(jnp.bfloat16)
        d_attn = dot(gated, w_aug[...], NT).astype(jnp.bfloat16)
        gt = [d_attn[:, j * LANES : (j + 1) * LANES] for j in range(tiles)]
        results = [[jnp.zeros((rows, LANES), jnp.float32) for _ in range(tiles)] for _ in range(4)]
        for h in range(heads):
            first = h * HEAD_DIM // LANES
            last = (h * HEAD_DIM + HEAD_DIM - 1) // LANES
            span = range(first, last + 1)
            mask = head_of[:, first * LANES : (last + 1) * LANES] == h
            ones = jnp.where(mask, 1.0, 0.0)
            keep = ones.astype(jnp.bfloat16)

            def window(parts):
                return jnp.concatenate([parts[j] for j in span], axis=1)

            qw, kw, vw, gw = window(qt), window(kt), window(vt), window(gt)
            gm = gw * keep
            scores = dot(qw * keep, kw, NT) * factor
            scores = jnp.where(same, scores, -1e30)
            peak = jnp.max(scores, axis=-1, keepdims=True)
            expon = jnp.exp(scores - peak)
            probs = expon / jnp.sum(expon, axis=-1, keepdims=True)
            probs_b = probs.astype(jnp.bfloat16)
            out_w = dot(probs_b, vw)
            dv_w = dot(probs_b, gw, TN)
            dprobs = dot(gm, vw, NT)
            out_b = out_w.astype(jnp.bfloat16).astype(jnp.float32)
            delta = jnp.sum(gm.astype(jnp.float32) * out_b, axis=-1, keepdims=True)
            dscores = (probs * (dprobs - delta) * factor).astype(jnp.bfloat16)
            dq_w = dot(dscores, kw)
            dk_w = dot(dscores, qw, TN)
            for which, value in enumerate((dq_w, dk_w, dv_w, out_w)):
                for i, j in enumerate(span):
                    at = slice(i * LANES, (i + 1) * LANES)
                    results[which][j] = jnp.where(mask[:, at], value[:, at], results[which][j])
        for which in range(3):
            for j in range(full):
                at = pl.multiple_of(j * block_pos + start, group)
                out_pack[which, :, pl.ds(at, group), :] = (
                    results[which][j].astype(jnp.bfloat16).reshape(n, group, LANES)
                )
            old = out_pack[which, :, full * block_pos :, :].reshape(rows, LANES).astype(jnp.float32)
            out_pack[which, :, full * block_pos :, :] = (
                (old + results[which][full]).astype(jnp.bfloat16).reshape(n, group, LANES)
            )
        attn = jnp.concatenate(results[3], axis=1).astype(jnp.bfloat16)
        branch = dot(attn, w_aug[...])
        gate_own[...] += jnp.sum(grads * branch, axis=0, keepdims=True)
        return carry

    lax.fori_loop(0, groups, one_group, 0)

    for o in range(1, n):
        d = other(o)
        copy = remote(gate_own, gate_all.at[me], ps.at[d], pr.at[me], d)
        copy.start()
        started.append(copy)
        for a in range(3):
            copy = remote(out_pack.at[a, d], ret_pack.at[a, me], rs.at[a, d], rr.at[a, me], d)
            copy.start()
            started.append(copy)
    for a in range(3):
        ret_pack[a, me] = out_pack[a, me]
    gate_all[me] = gate_own[...]

    for o in range(1, n):
        s = other(o)
        remote(gate_own, gate_all.at[s], ps.at[s], pr.at[s], s).wait_recv()
    total = gate_all[0]
    for s in range(1, n):
        total += gate_all[s]
    gg_ref[...] = total
    for a, ref in enumerate((dq_ref, dk_ref, dv_ref)):
        for o in range(1, n):
            s = other(o)
            remote(ret_pack.at[a, s], ret_pack.at[a, s], rs.at[a, s], rr.at[a, s], s).wait_recv()
        for u in range(across_y):
            pieces = []
            for t in range(across_x):
                d = t * across_y + u
                for j in range(full):
                    pieces.append(ret_pack[a, d, j * block_pos : (j + 1) * block_pos, :])
                narrow = ret_pack[a, d, full * block_pos :, :]
                pieces.append(
                    jnp.concatenate([narrow[:, g * rest : (g + 1) * rest] for g in range(groups)], axis=0)
                )
            ref[u * block_pos : (u + 1) * block_pos, :] = jnp.concatenate(pieces, axis=1)
    for copy in started:
        copy.wait_send()


def per_device(query_states, key_states, value_states, grad_output, branch_gate, out_weight):
    across_x = lax.axis_size("tx")
    across_y = lax.axis_size("ty")
    n = across_x * across_y
    frames_here, positions, width = grad_output.shape
    block_pos = positions // across_y
    block_width = width // across_x
    rest = block_width % LANES
    fits = (
        frames_here == 1
        and rest > 0
        and LANES % rest == 0
        and rest % 16 == 0
        and block_width % HEAD_DIM == 0
        and block_pos % (LANES // rest * 16) == 0
        and n * block_pos * rest // LANES <= 2 * LANES
        and width % LANES == 0
    )
    if not fits:
        return per_device_plain(
            query_states, key_states, value_states, grad_output, branch_gate, out_weight
        )
    group = block_pos * rest // LANES
    packed = block_pos * block_width // LANES
    bf16, f32 = jnp.bfloat16, jnp.float32
    dma = pltpu.SemaphoreType.DMA
    grads = jax.ShapeDtypeStruct((positions, width), bf16)
    vmem = pl.BlockSpec(memory_space=pltpu.VMEM)
    dq, dk, dv, gate = pl.pallas_call(
        functools.partial(fused_kernel, across_x, across_y, block_width, group),
        out_shape=(grads, grads, grads, jax.ShapeDtypeStruct((1, width), f32)),
        in_specs=[vmem] * 6,
        out_specs=(vmem,) * 4,
        scratch_shapes=[
            pltpu.VMEM((3, n, packed, LANES), bf16),
            pltpu.VMEM((3, n, packed, LANES), bf16),
            pltpu.VMEM((n, block_pos, width), bf16),
            pltpu.VMEM((3, n, packed, LANES), bf16),
            pltpu.VMEM((3, n, packed, LANES), bf16),
            pltpu.VMEM(((block_width // LANES + 1) * LANES, width), bf16),
            pltpu.VMEM((1, width), f32),
            pltpu.VMEM((n, 1, width), f32),
            dma((3, n)), dma((3, n)), dma((n,)), dma((n,)),
            dma((3, n)), dma((3, n)), dma((n,)), dma((n,)),
        ],
        compiler_params=pltpu.CompilerParams(collective_id=0, has_side_effects=True),
    )(
        query_states[0], key_states[0], value_states[0],
        grad_output.reshape(across_y, block_pos, width),
        branch_gate.reshape(1, width), out_weight,
    )
    return dq[None], dk[None], dv[None], gate.reshape(width)


def solution(mesh):
    in_specs = (
        P(("clip", "tx", "ty"), None, None),
        P(("clip", "tx", "ty"), None, None),
        P(("clip", "tx", "ty"), None, None),
        P(("clip", "tx", "ty"), None, None),
        P("clip"),
        P("tx", None),
    )
    out_specs = (
        P(("clip", "tx", "ty"), None, None),
        P(("clip", "tx", "ty"), None, None),
        P(("clip", "tx", "ty"), None, None),
        P("clip"),
    )
    return jax.shard_map(
        per_device, mesh=mesh, in_specs=in_specs, out_specs=out_specs, check_vma=False
    )
```

```python
import functools

import jax
import jax.numpy as jnp
from jax import lax
from jax.experimental import pallas as pl
from jax.experimental.pallas import tpu as pltpu
from jax.sharding import PartitionSpec as P

HEAD_DIM = 72


def shortened(x):

    def short(part):
        return part.astype(jnp.bfloat16) if part.dtype == jnp.float32 else part

    return jax.tree.map(short, x)


def attend_block(queries, keys_in, values_in, grads_in):
    frames, block_pos, block_width = queries.shape
    heads_here = block_width // HEAD_DIM
    shape4 = (frames, block_pos, heads_here, HEAD_DIM)
    q_four = queries.reshape(shape4)
    k_four = keys_in.reshape(shape4)
    v_four = values_in.reshape(shape4)
    g_four = grads_in.reshape(shape4)
    factor = HEAD_DIM ** (-0.5)
    scores = (
        jnp.einsum("fphd,gphd->phfg", q_four, k_four, preferred_element_type=jnp.float32) * factor
    )
    peak = jnp.max(scores, axis=-1, keepdims=True)
    expon = jnp.exp(scores - peak)
    probs = expon / jnp.sum(expon, axis=-1, keepdims=True)
    probs_b = probs.astype(jnp.bfloat16)
    attn_out = jnp.einsum(
        "phfg,gphd->fphd", probs_b, v_four, preferred_element_type=jnp.float32
    ).astype(jnp.bfloat16)
    value_grad = jnp.einsum(
        "phfg,fphd->gphd", probs_b, g_four, preferred_element_type=jnp.float32
    ).astype(jnp.bfloat16)
    dprobs = jnp.einsum("fphd,gphd->phfg", g_four, v_four, preferred_element_type=jnp.float32)
    delta = jnp.sum(g_four.astype(jnp.float32) * attn_out.astype(jnp.float32), axis=-1)
    delta = jnp.transpose(delta, (1, 2, 0))[..., None]
    dscores = (probs * (dprobs - delta) * factor).astype(jnp.bfloat16)
    query_grad = jnp.einsum(
        "phfg,gphd->fphd", dscores, k_four, preferred_element_type=jnp.float32
    ).astype(jnp.bfloat16)
    key_grad = jnp.einsum(
        "phfg,fphd->gphd", dscores, q_four, preferred_element_type=jnp.float32
    ).astype(jnp.bfloat16)
    flat = (frames, block_pos, block_width)
    return (
        query_grad.reshape(flat),
        key_grad.reshape(flat),
        value_grad.reshape(flat),
        attn_out.reshape(flat),
    )


def split_for_direct(array, across_x, across_y):
    positions, width = array.shape
    pieces = array.reshape(across_y, positions // across_y, across_x, width // across_x)
    pieces = jnp.transpose(pieces, (2, 0, 1, 3))
    return pieces.reshape(1, across_x * across_y, positions // across_y, width // across_x)


def join_from_direct(array, across_x, across_y):
    block_pos, block_width = (array.shape[2], array.shape[3])
    pieces = array.reshape(across_x, across_y, block_pos, block_width)
    pieces = jnp.transpose(pieces, (1, 2, 0, 3))
    return pieces.reshape(1, across_y * block_pos, across_x * block_width)


def per_device_plain(query_states, key_states, value_states, grad_output, branch_gate, out_weight):
    across_x = lax.axis_size("tx")
    across_y = lax.axis_size("ty")
    devices_here = across_x * across_y
    positions = grad_output.shape[1]
    width = grad_output.shape[2]
    block_pos = positions // across_y
    block_width = width // across_x
    grad_rows = grad_output[0]
    gated = (grad_rows.astype(jnp.float32) * branch_gate).astype(jnp.bfloat16)
    d_attn = lax.dot_general(
        gated,
        lax.all_gather(out_weight, "tx", axis=0, tiled=True),
        (((1,), (1,)), ((), ())),
        preferred_element_type=jnp.float32,
    )
    d_attn = d_attn.astype(jnp.bfloat16)
    sources = (query_states[0], key_states[0], value_states[0], d_attn)
    prepared = tuple((split_for_direct(arr, across_x, across_y) for arr in sources))
    moved = jax.tree.map(
        lambda part, own: part.astype(own.dtype),
        lax.all_to_all(shortened(prepared), ("tx", "ty"), split_axis=1, concat_axis=0, tiled=True),
        prepared,
    )
    moved = tuple((arr.reshape(devices_here, block_pos, block_width) for arr in moved))
    results = attend_block(moved[0], moved[1], moved[2], moved[3])
    outgoing = tuple((arr.reshape(devices_here, 1, block_pos, block_width) for arr in results))
    returned = jax.tree.map(
        lambda part, own: part.astype(own.dtype),
        lax.all_to_all(shortened(outgoing), ("tx", "ty"), split_axis=0, concat_axis=1, tiled=True),
        outgoing,
    )
    returned = tuple((join_from_direct(arr, across_x, across_y) for arr in returned))
    query_grad, key_grad, value_grad, attn_frame = returned
    attn_rows = attn_frame[0]
    branch_out = jnp.dot(
        attn_rows,
        lax.all_gather(out_weight, "tx", axis=0, tiled=True),
        preferred_element_type=jnp.float32,
    )
    local_terms = jnp.sum(grad_rows.astype(jnp.float32) * branch_out, axis=0)
    gate_grad = lax.psum(local_terms, ("tx", "ty"))
    return (query_grad, key_grad, value_grad, gate_grad)


LANES = 128
CHUNKS = 2
MESH = pl.DeviceIdType.MESH
NT = (((1,), (1,)), ((), ()))
TN = (((0,), (0,)), ((), ()))


def dot(a, b, dims=(((1,), (0,)), ((), ()))):
    return lax.dot_general(a, b, dims, preferred_element_type=jnp.float32)


def pack(rows, across_x, block_width, group):
    full = block_width // LANES
    rest = block_width % LANES
    groups = LANES // rest
    block_pos = group * groups
    blocks = []
    for t in range(across_x):
        base = t * block_width
        tiles = [rows[:, base + j * LANES : base + (j + 1) * LANES] for j in range(full)]
        narrow = rows[:, base + full * LANES : base + block_width]
        for u in range(rows.shape[0] // block_pos):
            start = u * block_pos
            parts = [tile[start : start + block_pos] for tile in tiles]
            parts.append(
                jnp.concatenate(
                    [narrow[start + g * group : start + (g + 1) * group] for g in range(groups)], axis=1
                )
            )
            blocks.append((t, u, parts))
    return blocks


def fused_kernel(
    across_x, across_y, block_width, group,
    q_ref, k_ref, v_ref, g_ref, gate_ref, w_ref,
    dq_ref, dk_ref, dv_ref, gg_ref,
    send0, send1, recv0, recv1, recv_g, out0, out1, ret0, ret1, w_aug, gate_own, gate_all,
    gs, gr, ws, s0s, s0r, s1s, s1r, r0s, r0r, r1s, r1r, ps, pr,
):
    n = across_x * across_y
    mx, my = lax.axis_index("tx"), lax.axis_index("ty")
    me = mx * across_y + my
    full = block_width // LANES
    rest = block_width % LANES
    groups = LANES // rest
    per_chunk = groups // CHUNKS
    part_pos = group * per_chunk
    body = full * part_pos
    tiles = full + 1
    rows = n * group
    heads = block_width // HEAD_DIM
    factor = HEAD_DIM ** (-0.5)
    sends, recvs = (send0, send1), (recv0, recv1)

    def ident(d):
        return {"tx": d // across_y, "ty": d % across_y}

    def other(o):
        return lax.rem(me + o, n)

    def remote(src, dst, ss, sr, d):
        return pltpu.make_async_remote_copy(
            src_ref=src, dst_ref=dst, send_sem=ss, recv_sem=sr, device_id=ident(d), device_id_type=MESH
        )

    barrier = pltpu.get_barrier_semaphore()
    for o in range(1, n):
        pl.semaphore_signal(barrier, inc=1, device_id=ident(other(o)), device_id_type=MESH)
    pl.semaphore_wait(barrier, n - 1)

    def span_of(c):
        return pl.ds(c * part_pos, part_pos)

    def own_grads(act):
        for c in range(CHUNKS):
            for i, step in enumerate((1, -1, 0)):
                for v in range(across_y):
                    u = lax.rem(my + v, across_y)
                    to = mx + step
                    if step == 0 and v == 0:
                        continue

                    @pl.when((to >= 0) & (to < across_x))
                    def _():
                        act(
                            remote(
                                g_ref.at[u, span_of(c)], recv_g.at[me, span_of(c)],
                                gs.at[c, i * across_y + v], gr.at[c, me], to * across_y + u,
                            )
                        )

    def frame_wait(f, c):
        here = recv_g.at[f, span_of(c)]
        remote(here, here, ws.at[c, f], gr.at[c, f], lax.rem(me + 1, n)).wait_recv()

    def moving(f, c, step):
        here = recv_g.at[f, span_of(c)]
        return remote(here, here, ws.at[c, f], gr.at[c, f], me + step * across_y)

    def relays(act):
        for s in range(1, across_x - 1):
            for c in range(CHUNKS):
                for step in (1, -1):
                    origin = mx - s * step
                    last = across_x - 1 if step == 1 else 0

                    @pl.when((origin >= 0) & (origin < across_x) & (mx != last))
                    def _():
                        for u in range(across_y):
                            act(origin * across_y + u, c, step)

    def relay(f, c, step):
        frame_wait(f, c)
        moving(f, c, step).start()

    own_grads(lambda copy: copy.start())
    for a, ref in enumerate((q_ref, k_ref, v_ref)):
        for t, u, parts in pack(ref[...], across_x, block_width, group):
            d = t * across_y + u
            for c in range(CHUNKS):
                for j in range(full):
                    sends[c][d, a, j * part_pos : (j + 1) * part_pos, :] = parts[j][
                        c * part_pos : (c + 1) * part_pos
                    ]
            send0[d, a, body:, :] = parts[full]
    relays(relay)

    started = []
    for c, (ss, sr) in enumerate(((s0s, s0r), (s1s, s1r))):
        for o in range(1, n):
            d = other(o)
            copy = remote(sends[c].at[d], recvs[c].at[me], ss.at[d], sr.at[me], d)
            copy.start()
            started.append(copy)
        recvs[c][me] = sends[c][me]
    recv_g[me] = g_ref[my]
    w_aug[: full * LANES, :] = w_ref[: full * LANES, :]
    for g in range(groups):
        w_aug[full * LANES + g * rest : full * LANES + (g + 1) * rest, :] = w_ref[full * LANES :, :]
    out1[:, :, body:, :] = jnp.zeros((3, n, group, LANES), jnp.bfloat16)
    gate_own[...] = jnp.zeros_like(gate_own)

    def arrive(c):
        for v in range(1, across_y):
            frame_wait(mx * across_y + lax.rem(my + v, across_y), c)
        for s in range(1, across_x):
            for step in (1, -1):
                origin = mx - s * step
                last = across_x - 1 if step == 1 else 0
                early = (mx != last) if s < across_x - 1 else (mx != mx)

                @pl.when((origin >= 0) & (origin < across_x) & jnp.logical_not(early))
                def _():
                    for u in range(across_y):
                        frame_wait(origin * across_y + u, c)
        ss, sr = ((s0s, s0r), (s1s, s1r))[c]
        for o in range(1, n):
            s = other(o)
            remote(recvs[c].at[s], recvs[c].at[s], ss.at[s], sr.at[s], s).wait_recv()

    lane = lax.broadcasted_iota(jnp.int32, (1, tiles * LANES), 1)
    row_pos = lax.broadcasted_iota(jnp.int32, (rows, rows), 0) % group
    col_pos = lax.broadcasted_iota(jnp.int32, (rows, rows), 1) % group
    same = row_pos == col_pos

    def one_group(c, i, carry):
        g = c * per_chunk + i
        start = pl.multiple_of(g * group, group)
        inner = pl.multiple_of(i * group, group)
        tail = lane - full * LANES
        channel = jnp.where(
            tail < 0, lane, jnp.where(tail // rest == g, full * LANES + tail % rest, block_width)
        )
        head_of = channel // HEAD_DIM

        def load(a):
            parts = []
            for j in range(full):
                at = pl.multiple_of(j * part_pos + inner, group)
                parts.append(recvs[c][:, a, pl.ds(at, group), :].reshape(rows, LANES))
            parts.append(recv0[:, a, body:, :].reshape(rows, LANES))
            return parts

        qt, kt, vt = load(0), load(1), load(2)
        grads = recv_g[:, pl.ds(start, group), :].reshape(rows, recv_g.shape[2]).astype(jnp.float32)
        gated = (grads * gate_ref[...]).astype(jnp.bfloat16)
        d_attn = dot(gated, w_aug[...], NT).astype(jnp.bfloat16)
        gt = [d_attn[:, j * LANES : (j + 1) * LANES] for j in range(tiles)]
        results = [[jnp.zeros((rows, LANES), jnp.float32) for _ in range(tiles)] for _ in range(4)]
        for h in range(heads):
            first = h * HEAD_DIM // LANES
            last = (h * HEAD_DIM + HEAD_DIM - 1) // LANES
            span = range(first, last + 1)
            mask = head_of[:, first * LANES : (last + 1) * LANES] == h
            ones = jnp.where(mask, 1.0, 0.0)
            keep = ones.astype(jnp.bfloat16)

            def window(parts):
                return jnp.concatenate([parts[j] for j in span], axis=1)

            qw, kw, vw, gw = window(qt), window(kt), window(vt), window(gt)
            gm = gw * keep
            scores = dot(qw * keep, kw, NT) * factor
            scores = jnp.where(same, scores, -1e30)
            peak = jnp.max(scores, axis=-1, keepdims=True)
            expon = jnp.exp(scores - peak)
            probs = expon / jnp.sum(expon, axis=-1, keepdims=True)
            probs_b = probs.astype(jnp.bfloat16)
            out_w = dot(probs_b, vw)
            dv_w = dot(probs_b, gw, TN)
            dprobs = dot(gm, vw, NT)
            out_b = out_w.astype(jnp.bfloat16).astype(jnp.float32)
            delta = jnp.sum(gm.astype(jnp.float32) * out_b, axis=-1, keepdims=True)
            dscores = (probs * (dprobs - delta) * factor).astype(jnp.bfloat16)
            dq_w = dot(dscores, kw)
            dk_w = dot(dscores, qw, TN)
            for which, value in enumerate((dq_w, dk_w, dv_w, out_w)):
                for i, j in enumerate(span):
                    at = slice(i * LANES, (i + 1) * LANES)
                    results[which][j] = jnp.where(mask[:, at], value[:, at], results[which][j])
        for which in range(3):
            for j in range(full):
                at = pl.ds(pl.multiple_of(j * part_pos + inner, group), group)
                value = results[which][j].astype(jnp.bfloat16).reshape(n, group, LANES)
                if c == 0:
                    out0[:, which, at, :] = value
                else:
                    out1[which, :, at, :] = value
            old = out1[which, :, body:, :].reshape(rows, LANES).astype(jnp.float32)
            out1[which, :, body:, :] = (
                (old + results[which][full]).astype(jnp.bfloat16).reshape(n, group, LANES)
            )
        attn = jnp.concatenate(results[3], axis=1).astype(jnp.bfloat16)
        branch = dot(attn, w_aug[...])
        gate_own[...] += jnp.sum(grads * branch, axis=0, keepdims=True)
        return carry

    arrive(0)
    lax.fori_loop(0, per_chunk, functools.partial(one_group, 0), 0)
    for o in range(1, n):
        d = other(o)
        copy = remote(out0.at[d], ret0.at[me], r0s.at[d], r0r.at[me], d)
        copy.start()
        started.append(copy)
    arrive(1)
    lax.fori_loop(0, per_chunk, functools.partial(one_group, 1), 0)
    for o in range(1, n):
        d = other(o)
        copy = remote(gate_own, gate_all.at[me], ps.at[d], pr.at[me], d)
        copy.start()
        started.append(copy)
    for a in range(3):
        for o in range(1, n):
            d = other(o)
            copy = remote(out1.at[a, d], ret1.at[a, me], r1s.at[a, d], r1r.at[a, me], d)
            copy.start()
            started.append(copy)
    ret0[me] = out0[me]
    for a in range(3):
        ret1[a, me] = out1[a, me]
    gate_all[me] = gate_own[...]

    for o in range(1, n):
        s = other(o)
        remote(gate_own, gate_all.at[s], ps.at[s], pr.at[s], s).wait_recv()
        remote(ret0.at[s], ret0.at[s], r0s.at[s], r0r.at[s], s).wait_recv()
    total = gate_all[0]
    for s in range(1, n):
        total += gate_all[s]
    gg_ref[...] = total
    for a, ref in enumerate((dq_ref, dk_ref, dv_ref)):
        for o in range(1, n):
            s = other(o)
            remote(ret1.at[a, s], ret1.at[a, s], r1s.at[a, s], r1r.at[a, s], s).wait_recv()
        for u in range(across_y):
            pieces = []
            for t in range(across_x):
                d = t * across_y + u
                for j in range(full):
                    at = slice(j * part_pos, (j + 1) * part_pos)
                    pieces.append(jnp.concatenate([ret0[d, a, at, :], ret1[a, d, at, :]], axis=0))
                narrow = ret1[a, d, body:, :]
                pieces.append(
                    jnp.concatenate([narrow[:, g * rest : (g + 1) * rest] for g in range(groups)], axis=0)
                )
            at = slice(u * part_pos * CHUNKS, (u + 1) * part_pos * CHUNKS)
            ref[at, :] = jnp.concatenate(pieces, axis=1)
    for copy in started:
        copy.wait_send()
    own_grads(lambda copy: copy.wait_send())
    relays(lambda f, c, step: moving(f, c, step).wait_send())


def per_device(query_states, key_states, value_states, grad_output, branch_gate, out_weight):
    across_x = lax.axis_size("tx")
    across_y = lax.axis_size("ty")
    n = across_x * across_y
    frames_here, positions, width = grad_output.shape
    block_pos = positions // across_y
    block_width = width // across_x
    rest = block_width % LANES
    fits = (
        frames_here == 1
        and rest > 0
        and LANES % rest == 0
        and LANES // rest % CHUNKS == 0
        and rest % 16 == 0
        and block_width % HEAD_DIM == 0
        and block_pos % (LANES // rest * 16) == 0
        and n * block_pos * rest // LANES <= 2 * LANES
        and width % LANES == 0
    )
    if not fits:
        return per_device_plain(
            query_states, key_states, value_states, grad_output, branch_gate, out_weight
        )
    group = block_pos * rest // LANES
    body = block_pos // CHUNKS * (block_width // LANES)
    bf16, f32 = jnp.bfloat16, jnp.float32
    dma = pltpu.SemaphoreType.DMA
    grads = jax.ShapeDtypeStruct((positions, width), bf16)
    vmem = pl.BlockSpec(memory_space=pltpu.VMEM)
    dq, dk, dv, gate = pl.pallas_call(
        functools.partial(fused_kernel, across_x, across_y, block_width, group),
        out_shape=(grads, grads, grads, jax.ShapeDtypeStruct((1, width), f32)),
        in_specs=[vmem] * 6,
        out_specs=(vmem,) * 4,
        scratch_shapes=[
            pltpu.VMEM((n, 3, body + group, LANES), bf16),
            pltpu.VMEM((n, 3, body, LANES), bf16),
            pltpu.VMEM((n, 3, body + group, LANES), bf16),
            pltpu.VMEM((n, 3, body, LANES), bf16),
            pltpu.VMEM((n, block_pos, width), bf16),
            pltpu.VMEM((n, 3, body, LANES), bf16),
            pltpu.VMEM((3, n, body + group, LANES), bf16),
            pltpu.VMEM((n, 3, body, LANES), bf16),
            pltpu.VMEM((3, n, body + group, LANES), bf16),
            pltpu.VMEM(((block_width // LANES + 1) * LANES, width), bf16),
            pltpu.VMEM((1, width), f32),
            pltpu.VMEM((n, 1, width), f32),
            dma((CHUNKS, 3 * across_y)), dma((CHUNKS, n)), dma((CHUNKS, n)),
            dma((n,)), dma((n,)), dma((n,)), dma((n,)), dma((n,)), dma((n,)),
            dma((3, n)), dma((3, n)), dma((n,)), dma((n,)),
        ],
        compiler_params=pltpu.CompilerParams(collective_id=0, has_side_effects=True),
    )(
        query_states[0], key_states[0], value_states[0],
        grad_output.reshape(across_y, block_pos, width),
        branch_gate.reshape(1, width), out_weight,
    )
    return dq[None], dk[None], dv[None], gate.reshape(width)


def solution(mesh):
    in_specs = (
        P(("clip", "tx", "ty"), None, None),
        P(("clip", "tx", "ty"), None, None),
        P(("clip", "tx", "ty"), None, None),
        P(("clip", "tx", "ty"), None, None),
        P("clip"),
        P("tx", None),
    )
    out_specs = (
        P(("clip", "tx", "ty"), None, None),
        P(("clip", "tx", "ty"), None, None),
        P(("clip", "tx", "ty"), None, None),
        P("clip"),
    )
    return jax.shard_map(
        per_device, mesh=mesh, in_specs=in_specs, out_specs=out_specs, check_vma=False
    )
```

```python
import functools

import jax
import jax.numpy as jnp
from jax import lax
from jax.experimental import pallas as pl
from jax.experimental.pallas import tpu as pltpu
from jax.sharding import PartitionSpec as P

HEAD_DIM = 72


def shortened(x):

    def short(part):
        return part.astype(jnp.bfloat16) if part.dtype == jnp.float32 else part

    return jax.tree.map(short, x)


def attend_block(queries, keys_in, values_in, grads_in):
    frames, block_pos, block_width = queries.shape
    heads_here = block_width // HEAD_DIM
    shape4 = (frames, block_pos, heads_here, HEAD_DIM)
    q_four = queries.reshape(shape4)
    k_four = keys_in.reshape(shape4)
    v_four = values_in.reshape(shape4)
    g_four = grads_in.reshape(shape4)
    factor = HEAD_DIM ** (-0.5)
    scores = (
        jnp.einsum("fphd,gphd->phfg", q_four, k_four, preferred_element_type=jnp.float32) * factor
    )
    peak = jnp.max(scores, axis=-1, keepdims=True)
    expon = jnp.exp(scores - peak)
    probs = expon / jnp.sum(expon, axis=-1, keepdims=True)
    probs_b = probs.astype(jnp.bfloat16)
    attn_out = jnp.einsum(
        "phfg,gphd->fphd", probs_b, v_four, preferred_element_type=jnp.float32
    ).astype(jnp.bfloat16)
    value_grad = jnp.einsum(
        "phfg,fphd->gphd", probs_b, g_four, preferred_element_type=jnp.float32
    ).astype(jnp.bfloat16)
    dprobs = jnp.einsum("fphd,gphd->phfg", g_four, v_four, preferred_element_type=jnp.float32)
    delta = jnp.sum(g_four.astype(jnp.float32) * attn_out.astype(jnp.float32), axis=-1)
    delta = jnp.transpose(delta, (1, 2, 0))[..., None]
    dscores = (probs * (dprobs - delta) * factor).astype(jnp.bfloat16)
    query_grad = jnp.einsum(
        "phfg,gphd->fphd", dscores, k_four, preferred_element_type=jnp.float32
    ).astype(jnp.bfloat16)
    key_grad = jnp.einsum(
        "phfg,fphd->gphd", dscores, q_four, preferred_element_type=jnp.float32
    ).astype(jnp.bfloat16)
    flat = (frames, block_pos, block_width)
    return (
        query_grad.reshape(flat),
        key_grad.reshape(flat),
        value_grad.reshape(flat),
        attn_out.reshape(flat),
    )


def split_for_direct(array, across_x, across_y):
    positions, width = array.shape
    pieces = array.reshape(across_y, positions // across_y, across_x, width // across_x)
    pieces = jnp.transpose(pieces, (2, 0, 1, 3))
    return pieces.reshape(1, across_x * across_y, positions // across_y, width // across_x)


def join_from_direct(array, across_x, across_y):
    block_pos, block_width = (array.shape[2], array.shape[3])
    pieces = array.reshape(across_x, across_y, block_pos, block_width)
    pieces = jnp.transpose(pieces, (1, 2, 0, 3))
    return pieces.reshape(1, across_y * block_pos, across_x * block_width)


def per_device_plain(query_states, key_states, value_states, grad_output, branch_gate, out_weight):
    across_x = lax.axis_size("tx")
    across_y = lax.axis_size("ty")
    devices_here = across_x * across_y
    positions = grad_output.shape[1]
    width = grad_output.shape[2]
    block_pos = positions // across_y
    block_width = width // across_x
    grad_rows = grad_output[0]
    gated = (grad_rows.astype(jnp.float32) * branch_gate).astype(jnp.bfloat16)
    d_attn = lax.dot_general(
        gated,
        lax.all_gather(out_weight, "tx", axis=0, tiled=True),
        (((1,), (1,)), ((), ())),
        preferred_element_type=jnp.float32,
    )
    d_attn = d_attn.astype(jnp.bfloat16)
    sources = (query_states[0], key_states[0], value_states[0], d_attn)
    prepared = tuple((split_for_direct(arr, across_x, across_y) for arr in sources))
    moved = jax.tree.map(
        lambda part, own: part.astype(own.dtype),
        lax.all_to_all(shortened(prepared), ("tx", "ty"), split_axis=1, concat_axis=0, tiled=True),
        prepared,
    )
    moved = tuple((arr.reshape(devices_here, block_pos, block_width) for arr in moved))
    results = attend_block(moved[0], moved[1], moved[2], moved[3])
    outgoing = tuple((arr.reshape(devices_here, 1, block_pos, block_width) for arr in results))
    returned = jax.tree.map(
        lambda part, own: part.astype(own.dtype),
        lax.all_to_all(shortened(outgoing), ("tx", "ty"), split_axis=0, concat_axis=1, tiled=True),
        outgoing,
    )
    returned = tuple((join_from_direct(arr, across_x, across_y) for arr in returned))
    query_grad, key_grad, value_grad, attn_frame = returned
    attn_rows = attn_frame[0]
    branch_out = jnp.dot(
        attn_rows,
        lax.all_gather(out_weight, "tx", axis=0, tiled=True),
        preferred_element_type=jnp.float32,
    )
    local_terms = jnp.sum(grad_rows.astype(jnp.float32) * branch_out, axis=0)
    gate_grad = lax.psum(local_terms, ("tx", "ty"))
    return (query_grad, key_grad, value_grad, gate_grad)


LANES = 128
CHUNKS = 2
MESH = pl.DeviceIdType.MESH
NT = (((1,), (1,)), ((), ()))
TN = (((0,), (0,)), ((), ()))


def dot(a, b, dims=(((1,), (0,)), ((), ()))):
    return lax.dot_general(a, b, dims, preferred_element_type=jnp.float32)


def pack(rows, across_x, block_width, group):
    full = block_width // LANES
    rest = block_width % LANES
    groups = LANES // rest
    block_pos = group * groups
    blocks = []
    for t in range(across_x):
        base = t * block_width
        tiles = [rows[:, base + j * LANES : base + (j + 1) * LANES] for j in range(full)]
        narrow = rows[:, base + full * LANES : base + block_width]
        for u in range(rows.shape[0] // block_pos):
            start = u * block_pos
            parts = [tile[start : start + block_pos] for tile in tiles]
            parts.append(
                jnp.concatenate(
                    [narrow[start + g * group : start + (g + 1) * group] for g in range(groups)], axis=1
                )
            )
            blocks.append((t, u, parts))
    return blocks


def fused_kernel(
    across_x, across_y, block_width, group,
    q_hbm, k_hbm, v_hbm, g_hbm, gate_ref, w_hbm,
    dq_ref, dk_ref, dv_ref, gg_ref,
    q_ref, k_ref, v_ref, g_ref, w_ref, done_ref, send0, send1, recv0, recv1, recv_g, out0, out1, ret0, ret1, w_aug, gate_own, gate_all,
    load_sem, store_sem, gs, gr, ws, s0s, s0r, s1s, s1r, r0s, r0r, r1s, r1r, ps, pr,
):
    n = across_x * across_y
    mx, my = lax.axis_index("tx"), lax.axis_index("ty")
    me = mx * across_y + my
    full = block_width // LANES
    rest = block_width % LANES
    groups = LANES // rest
    per_chunk = groups // CHUNKS
    part_pos = group * per_chunk
    body = full * part_pos
    tiles = full + 1
    rows = n * group
    heads = block_width // HEAD_DIM
    factor = HEAD_DIM ** (-0.5)
    sends, recvs = (send0, send1), (recv0, recv1)

    def ident(d):
        return {"tx": d // across_y, "ty": d % across_y}

    def other(o):
        return lax.rem(me + o, n)

    def remote(src, dst, ss, sr, d):
        return pltpu.make_async_remote_copy(
            src_ref=src, dst_ref=dst, send_sem=ss, recv_sem=sr, device_id=ident(d), device_id_type=MESH
        )

    loads = []
    for i, (src, dst) in enumerate(
        ((g_hbm, g_ref), (q_hbm, q_ref), (k_hbm, k_ref), (v_hbm, v_ref), (w_hbm, w_ref))
    ):
        loads.append(pltpu.make_async_copy(src, dst, load_sem.at[i]))
        loads[-1].start()

    barrier = pltpu.get_barrier_semaphore()
    for o in range(1, n):
        pl.semaphore_signal(barrier, inc=1, device_id=ident(other(o)), device_id_type=MESH)
    pl.semaphore_wait(barrier, n - 1)

    def span_of(c):
        return pl.ds(c * part_pos, part_pos)

    def own_grads(act):
        for c in range(CHUNKS):
            for i, step in enumerate((1, -1, 0)):
                for v in range(across_y):
                    u = lax.rem(my + v, across_y)
                    to = mx + step
                    if step == 0 and v == 0:
                        continue

                    @pl.when((to >= 0) & (to < across_x))
                    def _():
                        act(
                            remote(
                                g_ref.at[u, span_of(c)], recv_g.at[me, span_of(c)],
                                gs.at[c, i * across_y + v], gr.at[c, me], to * across_y + u,
                            )
                        )

    def frame_wait(f, c):
        here = recv_g.at[f, span_of(c)]
        remote(here, here, ws.at[c, f], gr.at[c, f], lax.rem(me + 1, n)).wait_recv()

    def moving(f, c, step):
        here = recv_g.at[f, span_of(c)]
        return remote(here, here, ws.at[c, f], gr.at[c, f], me + step * across_y)

    def relays(act):
        for s in range(1, across_x - 1):
            for c in range(CHUNKS):
                for step in (1, -1):
                    origin = mx - s * step
                    last = across_x - 1 if step == 1 else 0

                    @pl.when((origin >= 0) & (origin < across_x) & (mx != last))
                    def _():
                        for u in range(across_y):
                            act(origin * across_y + u, c, step)

    def relay(f, c, step):
        frame_wait(f, c)
        moving(f, c, step).start()

    loads[0].wait()
    own_grads(lambda copy: copy.start())
    for a, ref in enumerate((q_ref, k_ref, v_ref)):
        loads[1 + a].wait()
        for t, u, parts in pack(ref[...], across_x, block_width, group):
            d = t * across_y + u
            for c in range(CHUNKS):
                for j in range(full):
                    sends[c][d, a, j * part_pos : (j + 1) * part_pos, :] = parts[j][
                        c * part_pos : (c + 1) * part_pos
                    ]
            send0[d, a, body:, :] = parts[full]
    relays(relay)

    started = []
    for c, (ss, sr) in enumerate(((s0s, s0r), (s1s, s1r))):
        for o in range(1, n):
            d = other(o)
            copy = remote(sends[c].at[d], recvs[c].at[me], ss.at[d], sr.at[me], d)
            copy.start()
            started.append(copy)
        recvs[c][me] = sends[c][me]
    recv_g[me] = g_ref[my]
    loads[4].wait()
    w_aug[: full * LANES, :] = w_ref[: full * LANES, :]
    for g in range(groups):
        w_aug[full * LANES + g * rest : full * LANES + (g + 1) * rest, :] = w_ref[full * LANES :, :]
    out1[:, :, body:, :] = jnp.zeros((3, n, group, LANES), jnp.bfloat16)
    gate_own[...] = jnp.zeros_like(gate_own)

    def arrive(c):
        for v in range(1, across_y):
            frame_wait(mx * across_y + lax.rem(my + v, across_y), c)
        for s in range(1, across_x):
            for step in (1, -1):
                origin = mx - s * step
                last = across_x - 1 if step == 1 else 0
                early = (mx != last) if s < across_x - 1 else (mx != mx)

                @pl.when((origin >= 0) & (origin < across_x) & jnp.logical_not(early))
                def _():
                    for u in range(across_y):
                        frame_wait(origin * across_y + u, c)
        ss, sr = ((s0s, s0r), (s1s, s1r))[c]
        for o in range(1, n):
            s = other(o)
            remote(recvs[c].at[s], recvs[c].at[s], ss.at[s], sr.at[s], s).wait_recv()

    lane = lax.broadcasted_iota(jnp.int32, (1, tiles * LANES), 1)
    row_pos = lax.broadcasted_iota(jnp.int32, (rows, rows), 0) % group
    col_pos = lax.broadcasted_iota(jnp.int32, (rows, rows), 1) % group
    same = row_pos == col_pos

    def one_group(c, i, carry):
        g = c * per_chunk + i
        start = pl.multiple_of(g * group, group)
        inner = pl.multiple_of(i * group, group)
        tail = lane - full * LANES
        channel = jnp.where(
            tail < 0, lane, jnp.where(tail // rest == g, full * LANES + tail % rest, block_width)
        )
        head_of = channel // HEAD_DIM

        def load(a):
            parts = []
            for j in range(full):
                at = pl.multiple_of(j * part_pos + inner, group)
                parts.append(recvs[c][:, a, pl.ds(at, group), :].reshape(rows, LANES))
            parts.append(recv0[:, a, body:, :].reshape(rows, LANES))
            return parts

        qt, kt, vt = load(0), load(1), load(2)
        grads = recv_g[:, pl.ds(start, group), :].reshape(rows, recv_g.shape[2]).astype(jnp.float32)
        gated = (grads * gate_ref[...].reshape(1, gate_ref.shape[0])).astype(jnp.bfloat16)
        d_attn = dot(gated, w_aug[...], NT).astype(jnp.bfloat16)
        gt = [d_attn[:, j * LANES : (j + 1) * LANES] for j in range(tiles)]
        results = [[jnp.zeros((rows, LANES), jnp.float32) for _ in range(tiles)] for _ in range(4)]
        for h in range(heads):
            first = h * HEAD_DIM // LANES
            last = (h * HEAD_DIM + HEAD_DIM - 1) // LANES
            span = range(first, last + 1)
            mask = head_of[:, first * LANES : (last + 1) * LANES] == h
            ones = jnp.where(mask, 1.0, 0.0)
            keep = ones.astype(jnp.bfloat16)

            def window(parts):
                return jnp.concatenate([parts[j] for j in span], axis=1)

            qw, kw, vw, gw = window(qt), window(kt), window(vt), window(gt)
            gm = gw * keep
            scores = dot(qw * keep, kw, NT) * factor
            scores = jnp.where(same, scores, -1e30)
            peak = jnp.max(scores, axis=-1, keepdims=True)
            expon = jnp.exp(scores - peak)
            probs = expon / jnp.sum(expon, axis=-1, keepdims=True)
            probs_b = probs.astype(jnp.bfloat16)
            out_w = dot(probs_b, vw)
            dv_w = dot(probs_b, gw, TN)
            dprobs = dot(gm, vw, NT)
            out_b = out_w.astype(jnp.bfloat16).astype(jnp.float32)
            delta = jnp.sum(gm.astype(jnp.float32) * out_b, axis=-1, keepdims=True)
            dscores = (probs * (dprobs - delta) * factor).astype(jnp.bfloat16)
            dq_w = dot(dscores, kw)
            dk_w = dot(dscores, qw, TN)
            for which, value in enumerate((dq_w, dk_w, dv_w, out_w)):
                for i, j in enumerate(span):
                    at = slice(i * LANES, (i + 1) * LANES)
                    results[which][j] = jnp.where(mask[:, at], value[:, at], results[which][j])
        for which in range(3):
            for j in range(full):
                at = pl.ds(pl.multiple_of(j * part_pos + inner, group), group)
                value = results[which][j].astype(jnp.bfloat16).reshape(n, group, LANES)
                if c == 0:
                    out0[:, which, at, :] = value
                else:
                    out1[which, :, at, :] = value
            old = out1[which, :, body:, :].reshape(rows, LANES).astype(jnp.float32)
            out1[which, :, body:, :] = (
                (old + results[which][full]).astype(jnp.bfloat16).reshape(n, group, LANES)
            )
        attn = jnp.concatenate(results[3], axis=1).astype(jnp.bfloat16)
        branch = dot(attn, w_aug[...])
        gate_own[...] += jnp.sum(grads * branch, axis=0, keepdims=True)
        return carry

    arrive(0)
    lax.fori_loop(0, per_chunk, functools.partial(one_group, 0), 0)
    for o in range(1, n):
        d = other(o)
        copy = remote(out0.at[d], ret0.at[me], r0s.at[d], r0r.at[me], d)
        copy.start()
        started.append(copy)
    arrive(1)
    lax.fori_loop(0, per_chunk, functools.partial(one_group, 1), 0)
    for o in range(1, n):
        d = other(o)
        copy = remote(gate_own, gate_all.at[me], ps.at[d], pr.at[me], d)
        copy.start()
        started.append(copy)
    for a in range(3):
        for o in range(1, n):
            d = other(o)
            copy = remote(out1.at[a, d], ret1.at[a, me], r1s.at[a, d], r1r.at[a, me], d)
            copy.start()
            started.append(copy)
    ret0[me] = out0[me]
    for a in range(3):
        ret1[a, me] = out1[a, me]
    gate_all[me] = gate_own[...]

    for o in range(1, n):
        s = other(o)
        remote(gate_own, gate_all.at[s], ps.at[s], pr.at[s], s).wait_recv()
        remote(ret0.at[s], ret0.at[s], r0s.at[s], r0r.at[s], s).wait_recv()
    total = gate_all[0]
    for s in range(1, n):
        total += gate_all[s]
    gg_ref[...] = total
    stores = []
    for a, ref in enumerate((dq_ref, dk_ref, dv_ref)):
        for o in range(1, n):
            s = other(o)
            remote(ret1.at[a, s], ret1.at[a, s], r1s.at[a, s], r1r.at[a, s], s).wait_recv()
        for u in range(across_y):
            pieces = []
            for t in range(across_x):
                d = t * across_y + u
                for j in range(full):
                    at = slice(j * part_pos, (j + 1) * part_pos)
                    pieces.append(jnp.concatenate([ret0[d, a, at, :], ret1[a, d, at, :]], axis=0))
                narrow = ret1[a, d, body:, :]
                pieces.append(
                    jnp.concatenate([narrow[:, g * rest : (g + 1) * rest] for g in range(groups)], axis=0)
                )
            at = slice(u * part_pos * CHUNKS, (u + 1) * part_pos * CHUNKS)
            done_ref[a, at, :] = jnp.concatenate(pieces, axis=1)
        stores.append(pltpu.make_async_copy(done_ref.at[a], ref, store_sem.at[a]))
        stores[-1].start()
    for copy in stores:
        copy.wait()
    for copy in started:
        copy.wait_send()
    own_grads(lambda copy: copy.wait_send())
    relays(lambda f, c, step: moving(f, c, step).wait_send())


def hand_over(dq_in, dk_in, dv_in, gate_in, dq_out, dk_out, dv_out, gate_out, held, in_sem, out_sem):
    pairs = ((dq_in, dq_out), (dk_in, dk_out), (dv_in, dv_out))
    ins = [pltpu.make_async_copy(src, held.at[i], in_sem.at[i]) for i, (src, _) in enumerate(pairs)]
    outs = [pltpu.make_async_copy(held.at[i], dst.at[0], out_sem.at[i]) for i, (_, dst) in enumerate(pairs)]
    for copy in ins:
        copy.start()
    gate_out[...] = gate_in[...].reshape(gate_out.shape)
    for i in range(3):
        ins[i].wait()
        outs[i].start()
    for copy in outs:
        copy.wait()


def per_device(query_states, key_states, value_states, grad_output, branch_gate, out_weight):
    across_x = lax.axis_size("tx")
    across_y = lax.axis_size("ty")
    n = across_x * across_y
    frames_here, positions, width = grad_output.shape
    block_pos = positions // across_y
    block_width = width // across_x
    rest = block_width % LANES
    fits = (
        frames_here == 1
        and rest > 0
        and LANES % rest == 0
        and LANES // rest % CHUNKS == 0
        and rest % 16 == 0
        and block_width % HEAD_DIM == 0
        and block_pos % (LANES // rest * 16) == 0
        and n * block_pos * rest // LANES <= 2 * LANES
        and width % LANES == 0
    )
    if not fits:
        return per_device_plain(
            query_states, key_states, value_states, grad_output, branch_gate, out_weight
        )
    group = block_pos * rest // LANES
    body = block_pos // CHUNKS * (block_width // LANES)
    bf16, f32 = jnp.bfloat16, jnp.float32
    dma = pltpu.SemaphoreType.DMA
    grads = jax.ShapeDtypeStruct((positions, width), bf16)
    vmem = pl.BlockSpec(memory_space=pltpu.VMEM)
    anywhere = pl.BlockSpec(memory_space=pl.ANY)
    dq, dk, dv, gate = pl.pallas_call(
        functools.partial(fused_kernel, across_x, across_y, block_width, group),
        out_shape=(grads, grads, grads, jax.ShapeDtypeStruct((1, width), f32)),
        in_specs=[anywhere] * 4 + [vmem, anywhere],
        out_specs=(anywhere,) * 3 + (vmem,),
        scratch_shapes=[
            pltpu.VMEM((positions, width), bf16),
            pltpu.VMEM((positions, width), bf16),
            pltpu.VMEM((positions, width), bf16),
            pltpu.VMEM((across_y, block_pos, width), bf16),
            pltpu.VMEM((block_width, width), bf16),
            pltpu.VMEM((3, positions, width), bf16),
            pltpu.VMEM((n, 3, body + group, LANES), bf16),
            pltpu.VMEM((n, 3, body, LANES), bf16),
            pltpu.VMEM((n, 3, body + group, LANES), bf16),
            pltpu.VMEM((n, 3, body, LANES), bf16),
            pltpu.VMEM((n, block_pos, width), bf16),
            pltpu.VMEM((n, 3, body, LANES), bf16),
            pltpu.VMEM((3, n, body + group, LANES), bf16),
            pltpu.VMEM((n, 3, body, LANES), bf16),
            pltpu.VMEM((3, n, body + group, LANES), bf16),
            pltpu.VMEM(((block_width // LANES + 1) * LANES, width), bf16),
            pltpu.VMEM((1, width), f32),
            pltpu.VMEM((n, 1, width), f32),
            dma((5,)), dma((3,)), dma((CHUNKS, 3 * across_y)), dma((CHUNKS, n)), dma((CHUNKS, n)),
            dma((n,)), dma((n,)), dma((n,)), dma((n,)), dma((n,)), dma((n,)),
            dma((3, n)), dma((3, n)), dma((n,)), dma((n,)),
        ],
        compiler_params=pltpu.CompilerParams(collective_id=0, has_side_effects=True),
    )(
        query_states[0], key_states[0], value_states[0],
        grad_output.reshape(across_y, block_pos, width),
        branch_gate, out_weight,
    )
    final = jax.ShapeDtypeStruct((1, positions, width), bf16)
    return pl.pallas_call(
        hand_over,
        out_shape=(final, final, final, jax.ShapeDtypeStruct((width,), f32)),
        in_specs=[anywhere] * 3 + [vmem],
        out_specs=(anywhere,) * 3 + (vmem,),
        scratch_shapes=[pltpu.VMEM((3, positions, width), bf16), dma((3,)), dma((3,))],
    )(dq, dk, dv, gate)


def solution(mesh):
    in_specs = (
        P(("clip", "tx", "ty"), None, None),
        P(("clip", "tx", "ty"), None, None),
        P(("clip", "tx", "ty"), None, None),
        P(("clip", "tx", "ty"), None, None),
        P("clip"),
        P("tx", None),
    )
    out_specs = (
        P(("clip", "tx", "ty"), None, None),
        P(("clip", "tx", "ty"), None, None),
        P(("clip", "tx", "ty"), None, None),
        P("clip"),
    )
    return jax.shard_map(
        per_device, mesh=mesh, in_specs=in_specs, out_specs=out_specs, check_vma=False
    )
```

```python
import functools

import jax
import jax.numpy as jnp
from jax import lax
from jax.experimental import pallas as pl
from jax.experimental.pallas import tpu as pltpu
from jax.sharding import PartitionSpec as P

HEAD_DIM = 72


def shortened(x):

    def short(part):
        return part.astype(jnp.bfloat16) if part.dtype == jnp.float32 else part

    return jax.tree.map(short, x)


def attend_block(queries, keys_in, values_in, grads_in):
    frames, block_pos, block_width = queries.shape
    heads_here = block_width // HEAD_DIM
    shape4 = (frames, block_pos, heads_here, HEAD_DIM)
    q_four = queries.reshape(shape4)
    k_four = keys_in.reshape(shape4)
    v_four = values_in.reshape(shape4)
    g_four = grads_in.reshape(shape4)
    factor = HEAD_DIM ** (-0.5)
    scores = (
        jnp.einsum("fphd,gphd->phfg", q_four, k_four, preferred_element_type=jnp.float32) * factor
    )
    peak = jnp.max(scores, axis=-1, keepdims=True)
    expon = jnp.exp(scores - peak)
    probs = expon / jnp.sum(expon, axis=-1, keepdims=True)
    probs_b = probs.astype(jnp.bfloat16)
    attn_out = jnp.einsum(
        "phfg,gphd->fphd", probs_b, v_four, preferred_element_type=jnp.float32
    ).astype(jnp.bfloat16)
    value_grad = jnp.einsum(
        "phfg,fphd->gphd", probs_b, g_four, preferred_element_type=jnp.float32
    ).astype(jnp.bfloat16)
    dprobs = jnp.einsum("fphd,gphd->phfg", g_four, v_four, preferred_element_type=jnp.float32)
    delta = jnp.sum(g_four.astype(jnp.float32) * attn_out.astype(jnp.float32), axis=-1)
    delta = jnp.transpose(delta, (1, 2, 0))[..., None]
    dscores = (probs * (dprobs - delta) * factor).astype(jnp.bfloat16)
    query_grad = jnp.einsum(
        "phfg,gphd->fphd", dscores, k_four, preferred_element_type=jnp.float32
    ).astype(jnp.bfloat16)
    key_grad = jnp.einsum(
        "phfg,fphd->gphd", dscores, q_four, preferred_element_type=jnp.float32
    ).astype(jnp.bfloat16)
    flat = (frames, block_pos, block_width)
    return (
        query_grad.reshape(flat),
        key_grad.reshape(flat),
        value_grad.reshape(flat),
        attn_out.reshape(flat),
    )


def split_for_direct(array, across_x, across_y):
    positions, width = array.shape
    pieces = array.reshape(across_y, positions // across_y, across_x, width // across_x)
    pieces = jnp.transpose(pieces, (2, 0, 1, 3))
    return pieces.reshape(1, across_x * across_y, positions // across_y, width // across_x)


def join_from_direct(array, across_x, across_y):
    block_pos, block_width = (array.shape[2], array.shape[3])
    pieces = array.reshape(across_x, across_y, block_pos, block_width)
    pieces = jnp.transpose(pieces, (1, 2, 0, 3))
    return pieces.reshape(1, across_y * block_pos, across_x * block_width)


def per_device_plain(query_states, key_states, value_states, grad_output, branch_gate, out_weight):
    across_x = lax.axis_size("tx")
    across_y = lax.axis_size("ty")
    devices_here = across_x * across_y
    positions = grad_output.shape[1]
    width = grad_output.shape[2]
    block_pos = positions // across_y
    block_width = width // across_x
    grad_rows = grad_output[0]
    gated = (grad_rows.astype(jnp.float32) * branch_gate).astype(jnp.bfloat16)
    d_attn = lax.dot_general(
        gated,
        lax.all_gather(out_weight, "tx", axis=0, tiled=True),
        (((1,), (1,)), ((), ())),
        preferred_element_type=jnp.float32,
    )
    d_attn = d_attn.astype(jnp.bfloat16)
    sources = (query_states[0], key_states[0], value_states[0], d_attn)
    prepared = tuple((split_for_direct(arr, across_x, across_y) for arr in sources))
    moved = jax.tree.map(
        lambda part, own: part.astype(own.dtype),
        lax.all_to_all(shortened(prepared), ("tx", "ty"), split_axis=1, concat_axis=0, tiled=True),
        prepared,
    )
    moved = tuple((arr.reshape(devices_here, block_pos, block_width) for arr in moved))
    results = attend_block(moved[0], moved[1], moved[2], moved[3])
    outgoing = tuple((arr.reshape(devices_here, 1, block_pos, block_width) for arr in results))
    returned = jax.tree.map(
        lambda part, own: part.astype(own.dtype),
        lax.all_to_all(shortened(outgoing), ("tx", "ty"), split_axis=0, concat_axis=1, tiled=True),
        outgoing,
    )
    returned = tuple((join_from_direct(arr, across_x, across_y) for arr in returned))
    query_grad, key_grad, value_grad, attn_frame = returned
    attn_rows = attn_frame[0]
    branch_out = jnp.dot(
        attn_rows,
        lax.all_gather(out_weight, "tx", axis=0, tiled=True),
        preferred_element_type=jnp.float32,
    )
    local_terms = jnp.sum(grad_rows.astype(jnp.float32) * branch_out, axis=0)
    gate_grad = lax.psum(local_terms, ("tx", "ty"))
    return (query_grad, key_grad, value_grad, gate_grad)


LANES = 128
CHUNKS = 2
MESH = pl.DeviceIdType.MESH
NT = (((1,), (1,)), ((), ()))
TN = (((0,), (0,)), ((), ()))


def dot(a, b, dims=(((1,), (0,)), ((), ()))):
    return lax.dot_general(a, b, dims, preferred_element_type=jnp.float32)


def pack(rows, across_x, block_width, group):
    full = block_width // LANES
    rest = block_width % LANES
    groups = LANES // rest
    block_pos = group * groups
    blocks = []
    for t in range(across_x):
        base = t * block_width
        tiles = [rows[:, base + j * LANES : base + (j + 1) * LANES] for j in range(full)]
        narrow = rows[:, base + full * LANES : base + block_width]
        for u in range(rows.shape[0] // block_pos):
            start = u * block_pos
            parts = [tile[start : start + block_pos] for tile in tiles]
            parts.append(
                jnp.concatenate(
                    [narrow[start + g * group : start + (g + 1) * group] for g in range(groups)], axis=1
                )
            )
            blocks.append((t, u, parts))
    return blocks


def fused_kernel(
    across_x, across_y, block_width, group,
    q_hbm, k_hbm, v_hbm, g_hbm, gate_ref, w_hbm,
    dq_ref, dk_ref, dv_ref, gg_ref,
    q_ref, k_ref, v_ref, g_ref, w_ref, done_ref, send0, send1, recv0, recv1, recv_g, out0, out1, ret0, ret1, w_aug, gate_own, gate_all,
    load_sem, store_sem, gs, gr, ws, s0s, s0r, s1s, s1r, r0s, r0r, r1s, r1r, ps, pr,
):
    n = across_x * across_y
    mx, my = lax.axis_index("tx"), lax.axis_index("ty")
    me = mx * across_y + my
    full = block_width // LANES
    rest = block_width % LANES
    groups = LANES // rest
    per_chunk = groups // CHUNKS
    part_pos = group * per_chunk
    body = full * part_pos
    tiles = full + 1
    rows = n * group
    heads = block_width // HEAD_DIM
    factor = HEAD_DIM ** (-0.5)
    sends, recvs = (send0, send1), (recv0, recv1)

    def ident(d):
        return {"tx": d // across_y, "ty": d % across_y}

    half = across_x // 2
    side = mx // half * half

    def other(o):
        near, i = (side, o - half * across_y) if o > half * across_y else (half - side, o - 1)
        to = near + lax.rem(mx + i // across_y, half)
        return to * across_y + lax.rem(my + i % across_y, across_y)

    def remote(src, dst, ss, sr, d):
        return pltpu.make_async_remote_copy(
            src_ref=src, dst_ref=dst, send_sem=ss, recv_sem=sr, device_id=ident(d), device_id_type=MESH
        )

    loads = []
    for i, (src, dst) in enumerate(
        ((g_hbm, g_ref), (q_hbm, q_ref), (k_hbm, k_ref), (v_hbm, v_ref), (w_hbm, w_ref))
    ):
        loads.append(pltpu.make_async_copy(src, dst, load_sem.at[i]))
        loads[-1].start()

    barrier = pltpu.get_barrier_semaphore()
    for o in range(1, n):
        pl.semaphore_signal(barrier, inc=1, device_id=ident(other(o)), device_id_type=MESH)
    pl.semaphore_wait(barrier, n - 1)

    def span_of(c):
        return pl.ds(c * part_pos, part_pos)

    def own_grads(act):
        for c in range(CHUNKS):
            for i, step in enumerate((1, -1, 0)):
                for v in range(across_y):
                    u = lax.rem(my + v, across_y)
                    to = mx + step
                    if step == 0 and v == 0:
                        continue

                    @pl.when((to >= 0) & (to < across_x))
                    def _():
                        act(
                            remote(
                                g_ref.at[u, span_of(c)], recv_g.at[me, span_of(c)],
                                gs.at[c, i * across_y + v], gr.at[c, me], to * across_y + u,
                            )
                        )

    def frame_wait(f, c):
        here = recv_g.at[f, span_of(c)]
        remote(here, here, ws.at[c, f], gr.at[c, f], lax.rem(me + 1, n)).wait_recv()

    def moving(f, c, step):
        here = recv_g.at[f, span_of(c)]
        return remote(here, here, ws.at[c, f], gr.at[c, f], me + step * across_y)

    def relays(act):
        for s in range(1, across_x - 1):
            for c in range(CHUNKS):
                for step in (1, -1):
                    origin = mx - s * step
                    last = across_x - 1 if step == 1 else 0

                    @pl.when((origin >= 0) & (origin < across_x) & (mx != last))
                    def _():
                        for u in range(across_y):
                            act(origin * across_y + u, c, step)

    def relay(f, c, step):
        frame_wait(f, c)
        moving(f, c, step).start()

    loads[0].wait()
    own_grads(lambda copy: copy.start())
    for a, ref in enumerate((q_ref, k_ref, v_ref)):
        loads[1 + a].wait()
        for t, u, parts in pack(ref[...], across_x, block_width, group):
            d = t * across_y + u
            for c in range(CHUNKS):
                for j in range(full):
                    sends[c][d, a, j * part_pos : (j + 1) * part_pos, :] = parts[j][
                        c * part_pos : (c + 1) * part_pos
                    ]
            send0[d, a, body:, :] = parts[full]
    relays(relay)

    started = []
    for c, (ss, sr) in enumerate(((s0s, s0r), (s1s, s1r))):
        for o in range(1, n):
            d = other(o)
            copy = remote(sends[c].at[d], recvs[c].at[me], ss.at[d], sr.at[me], d)
            copy.start()
            started.append(copy)
        recvs[c][me] = sends[c][me]
    recv_g[me] = g_ref[my]
    loads[4].wait()
    w_aug[: full * LANES, :] = w_ref[: full * LANES, :]
    for g in range(groups):
        w_aug[full * LANES + g * rest : full * LANES + (g + 1) * rest, :] = w_ref[full * LANES :, :]
    out1[:, :, body:, :] = jnp.zeros((3, n, group, LANES), jnp.bfloat16)
    gate_own[...] = jnp.zeros_like(gate_own)

    def arrive(c):
        for v in range(1, across_y):
            frame_wait(mx * across_y + lax.rem(my + v, across_y), c)
        for s in range(1, across_x):
            for step in (1, -1):
                origin = mx - s * step
                last = across_x - 1 if step == 1 else 0
                early = (mx != last) if s < across_x - 1 else (mx != mx)

                @pl.when((origin >= 0) & (origin < across_x) & jnp.logical_not(early))
                def _():
                    for u in range(across_y):
                        frame_wait(origin * across_y + u, c)
        ss, sr = ((s0s, s0r), (s1s, s1r))[c]
        for o in range(1, n):
            s = other(o)
            remote(recvs[c].at[s], recvs[c].at[s], ss.at[s], sr.at[s], s).wait_recv()

    lane = lax.broadcasted_iota(jnp.int32, (1, tiles * LANES), 1)
    row_pos = lax.broadcasted_iota(jnp.int32, (rows, rows), 0) % group
    col_pos = lax.broadcasted_iota(jnp.int32, (rows, rows), 1) % group
    same = row_pos == col_pos

    def one_group(c, i, carry):
        g = c * per_chunk + i
        start = pl.multiple_of(g * group, group)
        inner = pl.multiple_of(i * group, group)
        tail = lane - full * LANES
        channel = jnp.where(
            tail < 0, lane, jnp.where(tail // rest == g, full * LANES + tail % rest, block_width)
        )
        head_of = channel // HEAD_DIM

        def load(a):
            parts = []
            for j in range(full):
                at = pl.multiple_of(j * part_pos + inner, group)
                parts.append(recvs[c][:, a, pl.ds(at, group), :].reshape(rows, LANES))
            parts.append(recv0[:, a, body:, :].reshape(rows, LANES))
            return parts

        qt, kt, vt = load(0), load(1), load(2)
        grads = recv_g[:, pl.ds(start, group), :].reshape(rows, recv_g.shape[2]).astype(jnp.float32)
        gated = (grads * gate_ref[...].reshape(1, gate_ref.shape[0])).astype(jnp.bfloat16)
        d_attn = dot(gated, w_aug[...], NT).astype(jnp.bfloat16)
        gt = [d_attn[:, j * LANES : (j + 1) * LANES] for j in range(tiles)]
        results = [[jnp.zeros((rows, LANES), jnp.float32) for _ in range(tiles)] for _ in range(4)]
        for h in range(heads):
            first = h * HEAD_DIM // LANES
            last = (h * HEAD_DIM + HEAD_DIM - 1) // LANES
            span = range(first, last + 1)
            mask = head_of[:, first * LANES : (last + 1) * LANES] == h
            ones = jnp.where(mask, 1.0, 0.0)
            keep = ones.astype(jnp.bfloat16)

            def window(parts):
                return jnp.concatenate([parts[j] for j in span], axis=1)

            qw, kw, vw, gw = window(qt), window(kt), window(vt), window(gt)
            gm = gw * keep
            scores = dot(qw * keep, kw, NT) * factor
            scores = jnp.where(same, scores, -1e30)
            peak = jnp.max(scores, axis=-1, keepdims=True)
            expon = jnp.exp(scores - peak)
            probs = expon / jnp.sum(expon, axis=-1, keepdims=True)
            probs_b = probs.astype(jnp.bfloat16)
            out_w = dot(probs_b, vw)
            dv_w = dot(probs_b, gw, TN)
            dprobs = dot(gm, vw, NT)
            out_b = out_w.astype(jnp.bfloat16).astype(jnp.float32)
            delta = jnp.sum(gm.astype(jnp.float32) * out_b, axis=-1, keepdims=True)
            dscores = (probs * (dprobs - delta) * factor).astype(jnp.bfloat16)
            dq_w = dot(dscores, kw)
            dk_w = dot(dscores, qw, TN)
            for which, value in enumerate((dq_w, dk_w, dv_w, out_w)):
                for i, j in enumerate(span):
                    at = slice(i * LANES, (i + 1) * LANES)
                    results[which][j] = jnp.where(mask[:, at], value[:, at], results[which][j])
        for which in range(3):
            for j in range(full):
                at = pl.ds(pl.multiple_of(j * part_pos + inner, group), group)
                value = results[which][j].astype(jnp.bfloat16).reshape(n, group, LANES)
                if c == 0:
                    out0[:, which, at, :] = value
                else:
                    out1[which, :, at, :] = value
            old = out1[which, :, body:, :].reshape(rows, LANES).astype(jnp.float32)
            out1[which, :, body:, :] = (
                (old + results[which][full]).astype(jnp.bfloat16).reshape(n, group, LANES)
            )
        attn = jnp.concatenate(results[3], axis=1).astype(jnp.bfloat16)
        branch = dot(attn, w_aug[...])
        gate_own[...] += jnp.sum(grads * branch, axis=0, keepdims=True)
        return carry

    arrive(0)
    lax.fori_loop(0, per_chunk, functools.partial(one_group, 0), 0)
    for o in range(1, n):
        d = other(o)
        copy = remote(out0.at[d], ret0.at[me], r0s.at[d], r0r.at[me], d)
        copy.start()
        started.append(copy)
    arrive(1)
    lax.fori_loop(0, per_chunk, functools.partial(one_group, 1), 0)
    for o in range(1, n):
        d = other(o)
        copy = remote(gate_own, gate_all.at[me], ps.at[d], pr.at[me], d)
        copy.start()
        started.append(copy)
    for a in range(3):
        for o in range(1, n):
            d = other(o)
            copy = remote(out1.at[a, d], ret1.at[a, me], r1s.at[a, d], r1r.at[a, me], d)
            copy.start()
            started.append(copy)
    ret0[me] = out0[me]
    for a in range(3):
        ret1[a, me] = out1[a, me]
    gate_all[me] = gate_own[...]

    for o in range(1, n):
        s = other(o)
        remote(gate_own, gate_all.at[s], ps.at[s], pr.at[s], s).wait_recv()
        remote(ret0.at[s], ret0.at[s], r0s.at[s], r0r.at[s], s).wait_recv()
    total = gate_all[0]
    for s in range(1, n):
        total += gate_all[s]
    gg_ref[...] = total
    stores = []
    for a, ref in enumerate((dq_ref, dk_ref, dv_ref)):
        for o in range(1, n):
            s = other(o)
            remote(ret1.at[a, s], ret1.at[a, s], r1s.at[a, s], r1r.at[a, s], s).wait_recv()
        for u in range(across_y):
            pieces = []
            for t in range(across_x):
                d = t * across_y + u
                for j in range(full):
                    at = slice(j * part_pos, (j + 1) * part_pos)
                    pieces.append(jnp.concatenate([ret0[d, a, at, :], ret1[a, d, at, :]], axis=0))
                narrow = ret1[a, d, body:, :]
                pieces.append(
                    jnp.concatenate([narrow[:, g * rest : (g + 1) * rest] for g in range(groups)], axis=0)
                )
            at = slice(u * part_pos * CHUNKS, (u + 1) * part_pos * CHUNKS)
            done_ref[a, at, :] = jnp.concatenate(pieces, axis=1)
        stores.append(pltpu.make_async_copy(done_ref.at[a], ref, store_sem.at[a]))
        stores[-1].start()
    for copy in stores:
        copy.wait()
    for copy in started:
        copy.wait_send()
    own_grads(lambda copy: copy.wait_send())
    relays(lambda f, c, step: moving(f, c, step).wait_send())


def hand_over(dq_in, dk_in, dv_in, gate_in, dq_out, dk_out, dv_out, gate_out, held, in_sem, out_sem):
    pairs = ((dq_in, dq_out), (dk_in, dk_out), (dv_in, dv_out))
    ins = [pltpu.make_async_copy(src, held.at[i], in_sem.at[i]) for i, (src, _) in enumerate(pairs)]
    outs = [pltpu.make_async_copy(held.at[i], dst.at[0], out_sem.at[i]) for i, (_, dst) in enumerate(pairs)]
    for copy in ins:
        copy.start()
    gate_out[...] = gate_in[...].reshape(gate_out.shape)
    for i in range(3):
        ins[i].wait()
        outs[i].start()
    for copy in outs:
        copy.wait()


def per_device(query_states, key_states, value_states, grad_output, branch_gate, out_weight):
    across_x = lax.axis_size("tx")
    across_y = lax.axis_size("ty")
    n = across_x * across_y
    frames_here, positions, width = grad_output.shape
    block_pos = positions // across_y
    block_width = width // across_x
    rest = block_width % LANES
    fits = (
        frames_here == 1
        and rest > 0
        and LANES % rest == 0
        and LANES // rest % CHUNKS == 0
        and rest % 16 == 0
        and block_width % HEAD_DIM == 0
        and block_pos % (LANES // rest * 16) == 0
        and n * block_pos * rest // LANES <= 2 * LANES
        and width % LANES == 0
        and across_x % 2 == 0
    )
    if not fits:
        return per_device_plain(
            query_states, key_states, value_states, grad_output, branch_gate, out_weight
        )
    group = block_pos * rest // LANES
    body = block_pos // CHUNKS * (block_width // LANES)
    bf16, f32 = jnp.bfloat16, jnp.float32
    dma = pltpu.SemaphoreType.DMA
    grads = jax.ShapeDtypeStruct((positions, width), bf16)
    vmem = pl.BlockSpec(memory_space=pltpu.VMEM)
    anywhere = pl.BlockSpec(memory_space=pl.ANY)
    dq, dk, dv, gate = pl.pallas_call(
        functools.partial(fused_kernel, across_x, across_y, block_width, group),
        out_shape=(grads, grads, grads, jax.ShapeDtypeStruct((1, width), f32)),
        in_specs=[anywhere] * 4 + [vmem, anywhere],
        out_specs=(anywhere,) * 3 + (vmem,),
        scratch_shapes=[
            pltpu.VMEM((positions, width), bf16),
            pltpu.VMEM((positions, width), bf16),
            pltpu.VMEM((positions, width), bf16),
            pltpu.VMEM((across_y, block_pos, width), bf16),
            pltpu.VMEM((block_width, width), bf16),
            pltpu.VMEM((3, positions, width), bf16),
            pltpu.VMEM((n, 3, body + group, LANES), bf16),
            pltpu.VMEM((n, 3, body, LANES), bf16),
            pltpu.VMEM((n, 3, body + group, LANES), bf16),
            pltpu.VMEM((n, 3, body, LANES), bf16),
            pltpu.VMEM((n, block_pos, width), bf16),
            pltpu.VMEM((n, 3, body, LANES), bf16),
            pltpu.VMEM((3, n, body + group, LANES), bf16),
            pltpu.VMEM((n, 3, body, LANES), bf16),
            pltpu.VMEM((3, n, body + group, LANES), bf16),
            pltpu.VMEM(((block_width // LANES + 1) * LANES, width), bf16),
            pltpu.VMEM((1, width), f32),
            pltpu.VMEM((n, 1, width), f32),
            dma((5,)), dma((3,)), dma((CHUNKS, 3 * across_y)), dma((CHUNKS, n)), dma((CHUNKS, n)),
            dma((n,)), dma((n,)), dma((n,)), dma((n,)), dma((n,)), dma((n,)),
            dma((3, n)), dma((3, n)), dma((n,)), dma((n,)),
        ],
        compiler_params=pltpu.CompilerParams(collective_id=0, has_side_effects=True),
    )(
        query_states[0], key_states[0], value_states[0],
        grad_output.reshape(across_y, block_pos, width),
        branch_gate, out_weight,
    )
    final = jax.ShapeDtypeStruct((1, positions, width), bf16)
    return pl.pallas_call(
        hand_over,
        out_shape=(final, final, final, jax.ShapeDtypeStruct((width,), f32)),
        in_specs=[anywhere] * 3 + [vmem],
        out_specs=(anywhere,) * 3 + (vmem,),
        scratch_shapes=[pltpu.VMEM((3, positions, width), bf16), dma((3,)), dma((3,))],
    )(dq, dk, dv, gate)


def solution(mesh):
    in_specs = (
        P(("clip", "tx", "ty"), None, None),
        P(("clip", "tx", "ty"), None, None),
        P(("clip", "tx", "ty"), None, None),
        P(("clip", "tx", "ty"), None, None),
        P("clip"),
        P("tx", None),
    )
    out_specs = (
        P(("clip", "tx", "ty"), None, None),
        P(("clip", "tx", "ty"), None, None),
        P(("clip", "tx", "ty"), None, None),
        P("clip"),
    )
    return jax.shard_map(
        per_device, mesh=mesh, in_specs=in_specs, out_specs=out_specs, check_vma=False
    )
```
